256 devices in a mesh: member: 16 (over z, y_hi), band: 16 (over y_lo, x, core).
Axes of the slice: x: 4, y: 4 (y_hi: 2, y_lo: 2; y = y_hi * 2 + y_lo), z: 8, core: 2. Of those that a mesh axis runs over, the one named last changes fastest.
Arguments:
- spectral: float32 [256, 768, 768], P('member', 'band'), parts along dimension 0, may hold values from -6 to 6
- coupling: float32 [16384, 1024], P(('member', 'band')), parts along dimension 0, may hold values from 0.02 to 162, as said below
- quadratic: float32 [16384, 1024], P(('member', 'band')), parts along dimension 0, may hold values from -1.5 to 1.5
Outputs:
- tendency_spectral: float32 [256, 768, 768], P('member', 'band'), parts along dimension 0
The draws below stay inside these ranges and needn't reach their ends.
There are 16 independent parts, one for each index of `member`. The reference program is written for one: setup_inputs(seed, part) draws one part's arguments, and reference() takes and returns one part's arrays. A program takes and returns all parts, laid end to end along the dimension named above; each array names one. Nothing has to cross between parts.
Inputs may be any that keep to these rules, and one draw needn't show every extreme that they name: `coupling`: positive.
All inputs are finite; a program needn't handle non-finite values.
Results may differ from the reference program's by a relative error of at most 0.00008.
Values sent between devices are 32-bit elements; how exact they have to be, the bound alone decides.
No kernel may reach another device: no remote copies, remote signals or barrier semaphores. Data moves between devices by JAX's collectives and lax.ppermute only.
A program may use at most 128 MiB of HBM per device.

```python
import math
import jax
import jax.numpy as jnp
from jax import lax

N = 1024
LEVELS = 16
KS = 768


def draw_coupling(key, part):
    keys = jax.random.split(jax.random.fold_in(key, 11), 3)
    rows = jnp.arange(N, dtype=jnp.float32) / N
    row_noise = jax.random.uniform(keys[0], (N,), jnp.float32)
    col_noise = jax.random.uniform(keys[1], (N,), jnp.float32)
    trend = jnp.exp(jnp.log(3.0) * rows)
    cell = jax.random.uniform(keys[2], (N, N), jnp.float32, 0.5, 1.5)
    row_scale = trend * jnp.exp(jnp.log(10.0) * row_noise)
    col_scale = jnp.exp(jnp.log(10.0) * col_noise)
    return (row_scale[:, None] * col_scale[None, :] * cell / 10.0).astype(jnp.float32)


def block_levels(stream_key, extent, shards, smallest, largest):
    def one(dim, shards_of):
        steps = jax.random.uniform(jax.random.fold_in(jax.random.fold_in(stream_key, 6), dim), (shards_of,), jnp.float32, smallest / len(shards), largest / len(shards))
        return jnp.repeat(jnp.exp(steps), extent[dim] // shards_of).reshape((-1,) + (1,) * (len(extent) - dim - 1))

    gain = one(*shards[0])
    for cut in shards[1:]:
        gain = gain * one(*cut)
    return gain


def noise(stream_key, shape, deviation, most, cuts=(), kind=jnp.bfloat16):
    result = deviation * jax.random.normal(stream_key, shape, jnp.float32)
    if cuts:
        result = result * block_levels(stream_key, shape, cuts, -0.22, 0.18)
    return jnp.clip(result, -most, most).astype(kind)


def setup_inputs(seed: int = 0, part: int = 0) -> dict:
    seeds = jax.random.split(jax.random.key(seed), 4)
    part_splits = jax.random.split(jax.random.fold_in(seeds[3], part), 4)
    spectral = noise(part_splits[0], (LEVELS, KS, KS), 1.0, 6.0, ((1, 16),), jnp.float32)
    coupling = draw_coupling(jax.random.fold_in(jax.random.fold_in(seeds[3], part), 71), part)
    quadratic = noise(part_splits[2], (N, N), 0.25, 1.5, ((0, 16),), jnp.float32)
    return {"spectral": spectral, "coupling": coupling, "quadratic": quadratic}


def tables(cells, coeffs):
    half_count = coeffs // 2
    position = jnp.arange(cells, dtype=jnp.int32)
    column = jnp.arange(coeffs, dtype=jnp.int32)
    wavenumber = jnp.where(column < half_count, column, column - half_count)
    turns = position[:, None] * wavenumber[None, :] % cells
    angles = turns.astype(jnp.float32) * (2.0 * math.pi / cells)
    basis_table = jnp.where(column[None, :] < half_count, jnp.cos(angles), jnp.sin(angles))
    synthesis = basis_table / math.sqrt(half_count)
    factor = jnp.where(wavenumber == 0, 1.0, 2.0) * (math.sqrt(half_count) / cells)
    analysis = (basis_table * factor[None, :]).T
    return (synthesis, analysis)

def reference(spectral, coupling, quadratic):
    synthesis, analysis = tables(N, KS)
    high = lax.Precision.HIGHEST
    section = jnp.einsum('lab,yb->lay', spectral, synthesis, precision=high)
    grid = jnp.einsum('xa,lay->lyx', synthesis, section, precision=high)
    product = coupling[None] * grid
    energy = lax.optimization_barrier(jnp.mean(product * product, axis=(1, 2)))
    scaled = product / jnp.sqrt(energy + 1e-06)[:, None, None]
    tendency = scaled + quadratic[None] * scaled * scaled
    back = jnp.einsum('ax,lyx->lya', analysis, tendency, precision=high)
    return jnp.einsum('by,lya->lab', analysis, back, precision=high)
```

```python
import functools, math
import numpy as np
import jax
import jax.numpy as jnp
from jax import lax
from jax.experimental import pallas as pl
from jax.experimental.pallas import tpu as pltpu
from jax.sharding import Mesh
from jax.sharding import PartitionSpec as P

F32, BF16 = jnp.float32, jnp.bfloat16
LANES = 128

BAND = ("band_0", "band_1", "band_2")
MEMBER_BAND = ("member",) + BAND


def trig_table(cells, coeffs):
    half = coeffs // 2
    position = np.arange(cells)[:, None]
    column = np.arange(coeffs)[None, :]
    turns = position * (column % half) % cells
    angles = turns * (2.0 * np.pi / cells)
    return np.where(column < half, np.cos(angles), np.sin(angles)).astype(np.float32)


def split_table(table):
    high = table.astype(jnp.bfloat16)
    low = (table - high.astype(np.float32)).astype(jnp.bfloat16)
    return high, low


def split(value):
    high = value.astype(BF16)
    return high, (value - high.astype(F32)).astype(BF16)


def dot(a, b):
    return jnp.dot(a, b, preferred_element_type=F32)


def dot3(a_high, a_low, b_high, b_low):
    return dot(a_high, b_high) + dot(a_low, b_high) + dot(a_high, b_low)


def lane_halves(shape):
    return lax.broadcasted_iota(jnp.int32, shape, 1) < LANES // 2


def swap(a, b):
    left = lane_halves(a.shape)
    return (
        jnp.where(left, a, pltpu.roll(b, LANES // 2, 1)),
        jnp.where(left, pltpu.roll(a, LANES // 2, 1), b),
    )


def synth_y(levels, rows, bands, x_ref, th_ref, tl_ref, o_ref, xh, xl, acc):
    m = levels * rows
    high, low = split(x_ref[...].reshape(m, x_ref.shape[2]))
    xh[...] = high
    xl[...] = low

    @pl.loop(0, th_ref.shape[1] // 256)
    def _(j):
        cols = pl.ds(pl.multiple_of(j * 256, 256), 256)
        acc[...] = dot3(xh[...], xl[...], th_ref[:, cols], tl_ref[:, cols])
        for p in range(levels // 2):
            for h in range(2):
                a = acc[2 * p * rows : (2 * p + 1) * rows, h * LANES : (h + 1) * LANES]
                b = acc[(2 * p + 1) * rows : (2 * p + 2) * rows, h * LANES : (h + 1) * LANES]
                even, odd = swap(a, b)
                o_ref[4 * j + 2 * h, :, p * LANES : (p + 1) * LANES] = even
                o_ref[4 * j + 2 * h + 1, :, p * LANES : (p + 1) * LANES] = odd


def synth_x(r_ref, th_ref, tl_ref, c_ref, p_ref, e_ref, rh, rl):
    k = rh.shape[0]
    n = rh.shape[1]
    high, low = split(r_ref[...].reshape(k, n))
    rh[...] = high
    rl[...] = low
    e_ref[...] = jnp.zeros_like(e_ref)

    for j in range(n // 256):
        cols = slice(j * 256, (j + 1) * 256)
        p_ref[:, cols] = dot3(th_ref[...], tl_ref[...], rh[:, cols], rl[:, cols])
        for h in range(2):
            lanes = slice(j * 256 + h * LANES, j * 256 + (h + 1) * LANES)
            product = p_ref[:, lanes] * c_ref[...]
            p_ref[:, lanes] = product
            total = jnp.sum(product * product, axis=0, keepdims=True)
            for d in range(e_ref.shape[0]):
                e_ref[d, 2 * j + h : 2 * j + h + 1, :] = total


def group_sum(v):
    lane = lax.broadcasted_iota(jnp.int32, v.shape, 1)
    step = 1
    while step < LANES // 2:
        v = v + jnp.where(lane % (2 * step) < step, pltpu.roll(v, LANES - step, 1), pltpu.roll(v, step, 1))
        step *= 2
    return v


def analyse_x(points, p_ref, e_ref, q_ref, th_ref, tl_ref, o_ref, gh, gl, acc):
    m = acc.shape[0]
    n = p_ref.shape[1]
    rows = o_ref.shape[1]
    total = group_sum(jnp.sum(e_ref[...], axis=0))
    scale = lax.rsqrt(total * (1.0 / points) + 1e-06)
    half = m // 2
    row = lax.broadcasted_iota(jnp.int32, (m, 1), 0)
    weight = jnp.where(row % half == 0, 1.0, 2.0).astype(F32)
    for t in range(n // LANES):
        lanes = slice(t * LANES, (t + 1) * LANES)
        scaled = p_ref[:, lanes] * scale[t : t + 1, :]
        high, low = split(scaled + q_ref[...] * scaled * scaled)
        gh[:, lanes] = high
        gl[:, lanes] = low
    for j in range(n // 256):
        cols = slice(j * 256, (j + 1) * 256)
        value = dot3(th_ref[...], tl_ref[...], gh[:, cols], gl[:, cols]) * weight
        o_ref[:, :, cols] = value.reshape(m // rows, rows, 256)


def analyse_y(levels, factor, r_ref, th_ref, tl_ref, o_ref, yh, yl):
    bands, rows = r_ref.shape[0], r_ref.shape[1]
    for p in range(levels // 2):
        for s in range(bands // 2):
            a = r_ref[2 * s, :, p * LANES : (p + 1) * LANES]
            b = r_ref[2 * s + 1, :, p * LANES : (p + 1) * LANES]
            for i, piece in enumerate(swap(a, b)):
                high, low = split(piece)
                at = (2 * p + i) * rows
                yh[at : at + rows, s * LANES : (s + 1) * LANES] = high
                yl[at : at + rows, s * LANES : (s + 1) * LANES] = low
    coeffs = th_ref.shape[1]
    for j in range(coeffs // 256):
        cols = slice(j * 256, (j + 1) * 256)
        col = j * 256 + lax.broadcasted_iota(jnp.int32, (1, 256), 1)
        weight = jnp.where(col % (coeffs // 2) == 0, factor, 2.0 * factor).astype(F32)
        value = dot3(yh[...], yl[...], th_ref[:, cols], tl_ref[:, cols]) * weight
        o_ref[:, :, cols] = value.reshape(levels, rows, 256)


CHUNKS = 1


def stage(kernel, out_shape, scratch, flops, nbytes):
    return pl.pallas_call(
        kernel,
        out_shape=out_shape,
        scratch_shapes=scratch,
        compiler_params=pltpu.CompilerParams(vmem_limit_bytes=40 * 1024 * 1024),
        cost_estimate=pl.CostEstimate(flops=flops, bytes_accessed=nbytes, transcendentals=0),
    )


def on_device(bands, spectral, coupling, quadratic):
    levels, rows, coeffs = spectral.shape
    own, cells = coupling.shape
    table = trig_table(cells, coeffs)
    th, tl = (jnp.asarray(t) for t in split_table(table))
    uh, ul = (jnp.asarray(t) for t in split_table(np.ascontiguousarray(table.T)))
    count = levels // CHUNKS
    n = count * own
    flops = 6 * count * own * cells * coeffs
    nbytes = 4 * n * (cells + coeffs) + 4 * cells * coeffs
    ct = coupling.T * (1.0 / (coeffs // 2))
    ct = jnp.concatenate([ct, ct], axis=1)
    qt = jnp.concatenate([quadratic.T, quadratic.T], axis=1)
    factor = (coeffs // 2) / float(cells * cells)
    spread = jax.ShapeDtypeStruct((bands, rows, n), F32)

    def exchange(a):
        return lax.all_to_all(a, BAND, 0, 0, tiled=True)

    first = stage(
        functools.partial(synth_y, count, rows, bands),
        spread,
        [pltpu.VMEM((count * rows, coeffs), BF16)] * 2 + [pltpu.VMEM((count * rows, 256), F32)],
        flops, nbytes,
    )
    second = stage(
        synth_x,
        (jax.ShapeDtypeStruct((cells, n), F32), jax.ShapeDtypeStruct((bands, 8, LANES), F32)),
        [pltpu.VMEM((coeffs, n), BF16)] * 2,
        flops, nbytes,
    )
    third = stage(
        functools.partial(analyse_x, float(cells * cells)),
        spread,
        [pltpu.VMEM((cells, n), BF16)] * 2 + [pltpu.VMEM((coeffs, 256), F32)],
        flops, nbytes,
    )
    fourth = stage(
        functools.partial(analyse_y, count, factor),
        jax.ShapeDtypeStruct((count, rows, coeffs), F32),
        [pltpu.VMEM((count * rows, cells), BF16)] * 2,
        flops, nbytes,
    )
    done = []
    for k in range(CHUNKS):
        sent = first(spectral[k * count : (k + 1) * count], uh, ul)
        turned = exchange(sent)
        product, energy = second(turned, th, tl, ct)
        energy = exchange(energy)
        back = third(product, energy, qt, uh, ul)
        done.append(fourth(exchange(back), th, tl))
    return jnp.concatenate(done, axis=0) if CHUNKS > 1 else done[0]


def solution(mesh):
    torus = Mesh(
        mesh.devices.reshape(mesh.shape["member"], 2, 4, 2),
        ("member",) + BAND,
    )
    return jax.shard_map(
        functools.partial(on_device, mesh.shape["band"]),
        mesh=torus,
        in_specs=(P("member", BAND, None), P(MEMBER_BAND, None), P(MEMBER_BAND, None)),
        out_specs=P("member", BAND, None),
        check_vma=False,
    )
```

```python
import functools, math
import numpy as np
import jax
import jax.numpy as jnp
from jax import lax
from jax.experimental import pallas as pl
from jax.experimental.pallas import tpu as pltpu
from jax.sharding import Mesh
from jax.sharding import PartitionSpec as P

F32, BF16 = jnp.float32, jnp.bfloat16
LANES = 128

BAND = ("band_0", "band_1", "band_2")
MEMBER_BAND = ("member",) + BAND


def trig_table(cells, coeffs):
    half = coeffs // 2
    position = np.arange(cells)[:, None]
    column = np.arange(coeffs)[None, :]
    turns = position * (column % half) % cells
    angles = turns * (2.0 * np.pi / cells)
    return np.where(column < half, np.cos(angles), np.sin(angles)).astype(np.float32)


def split_table(table):
    high = table.astype(jnp.bfloat16)
    low = (table - high.astype(np.float32)).astype(jnp.bfloat16)
    return high, low


def split(value):
    high = value.astype(BF16)
    return high, (value - high.astype(F32)).astype(BF16)


def dot(a, b):
    return jnp.dot(a, b, preferred_element_type=F32)


def dot3(a_high, a_low, b_high, b_low):
    return dot(a_high, b_high) + dot(a_low, b_high) + dot(a_high, b_low)


def lane_halves(shape):
    return lax.broadcasted_iota(jnp.int32, shape, 1) < LANES // 2


def swap(a, b):
    left = lane_halves(a.shape)
    return (
        jnp.where(left, a, pltpu.roll(b, LANES // 2, 1)),
        jnp.where(left, pltpu.roll(a, LANES // 2, 1), b),
    )


def synth_y(levels, rows, bands, x_ref, th_ref, tl_ref, o_ref, xh, xl, acc):
    m = levels * rows
    high, low = split(x_ref[...].reshape(m, x_ref.shape[2]))
    xh[...] = high
    xl[...] = low

    @pl.loop(0, th_ref.shape[1] // 256)
    def _(j):
        cols = pl.ds(pl.multiple_of(j * 256, 256), 256)
        acc[...] = dot3(xh[...], xl[...], th_ref[:, cols], tl_ref[:, cols])
        for p in range(levels // 2):
            for h in range(2):
                a = acc[2 * p * rows : (2 * p + 1) * rows, h * LANES : (h + 1) * LANES]
                b = acc[(2 * p + 1) * rows : (2 * p + 2) * rows, h * LANES : (h + 1) * LANES]
                even, odd = swap(a, b)
                o_ref[4 * j + 2 * h, :, p * LANES : (p + 1) * LANES] = even
                o_ref[4 * j + 2 * h + 1, :, p * LANES : (p + 1) * LANES] = odd


def doubled_columns(a):
    return jnp.concatenate([a, a], axis=0).T


def synth_x(r_ref, th_ref, tl_ref, c_ref, p_ref, e_ref, rh, rl):
    k = rh.shape[0]
    n = rh.shape[1]
    coupling = doubled_columns(c_ref[...]) * (1.0 / (k // 2))
    high, low = split(r_ref[...].reshape(k, n))
    rh[...] = high
    rl[...] = low
    e_ref[...] = jnp.zeros_like(e_ref)

    for j in range(n // 256):
        cols = slice(j * 256, (j + 1) * 256)
        p_ref[:, cols] = dot3(th_ref[...], tl_ref[...], rh[:, cols], rl[:, cols])
        for h in range(2):
            lanes = slice(j * 256 + h * LANES, j * 256 + (h + 1) * LANES)
            product = p_ref[:, lanes] * coupling
            p_ref[:, lanes] = product
            total = jnp.sum(product * product, axis=0, keepdims=True)
            for d in range(e_ref.shape[0]):
                e_ref[d, 2 * j + h : 2 * j + h + 1, :] = total


def group_sum(v):
    lane = lax.broadcasted_iota(jnp.int32, v.shape, 1)
    step = 1
    while step < LANES // 2:
        v = v + jnp.where(lane % (2 * step) < step, pltpu.roll(v, LANES - step, 1), pltpu.roll(v, step, 1))
        step *= 2
    return v


def analyse_x(points, p_ref, e_ref, q_ref, th_ref, tl_ref, o_ref, gh, gl, acc):
    m = acc.shape[0]
    n = p_ref.shape[1]
    rows = o_ref.shape[1]
    quadratic = doubled_columns(q_ref[...])
    total = group_sum(jnp.sum(e_ref[...], axis=0))
    scale = lax.rsqrt(total * (1.0 / points) + 1e-06)
    half = m // 2
    row = lax.broadcasted_iota(jnp.int32, (m, 1), 0)
    weight = jnp.where(row % half == 0, 1.0, 2.0).astype(F32)
    for t in range(n // LANES):
        lanes = slice(t * LANES, (t + 1) * LANES)
        scaled = p_ref[:, lanes] * scale[t : t + 1, :]
        high, low = split(scaled + quadratic * scaled * scaled)
        gh[:, lanes] = high
        gl[:, lanes] = low
    for j in range(n // 256):
        cols = slice(j * 256, (j + 1) * 256)
        value = dot3(th_ref[...], tl_ref[...], gh[:, cols], gl[:, cols]) * weight
        o_ref[:, :, cols] = value.reshape(m // rows, rows, 256)


def analyse_y(levels, factor, r_ref, th_ref, tl_ref, o_ref, yh, yl):
    bands, rows = r_ref.shape[0], r_ref.shape[1]
    for p in range(levels // 2):
        for s in range(bands // 2):
            a = r_ref[2 * s, :, p * LANES : (p + 1) * LANES]
            b = r_ref[2 * s + 1, :, p * LANES : (p + 1) * LANES]
            for i, piece in enumerate(swap(a, b)):
                high, low = split(piece)
                at = (2 * p + i) * rows
                yh[at : at + rows, s * LANES : (s + 1) * LANES] = high
                yl[at : at + rows, s * LANES : (s + 1) * LANES] = low
    coeffs = th_ref.shape[1]
    for j in range(coeffs // 256):
        cols = slice(j * 256, (j + 1) * 256)
        col = j * 256 + lax.broadcasted_iota(jnp.int32, (1, 256), 1)
        weight = jnp.where(col % (coeffs // 2) == 0, factor, 2.0 * factor).astype(F32)
        value = dot3(yh[...], yl[...], th_ref[:, cols], tl_ref[:, cols]) * weight
        o_ref[:, :, cols] = value.reshape(levels, rows, 256)


CHUNKS = 1


def stage(kernel, out_shape, scratch, flops, nbytes):
    return pl.pallas_call(
        kernel,
        out_shape=out_shape,
        scratch_shapes=scratch,
        compiler_params=pltpu.CompilerParams(vmem_limit_bytes=16 * 1024 * 1024),
        cost_estimate=pl.CostEstimate(flops=flops, bytes_accessed=nbytes, transcendentals=0),
    )


def on_device(bands, spectral, coupling, quadratic):
    levels, rows, coeffs = spectral.shape
    own, cells = coupling.shape
    table = trig_table(cells, coeffs)
    th, tl = (jnp.asarray(t) for t in split_table(table))
    uh, ul = (jnp.asarray(t) for t in split_table(np.ascontiguousarray(table.T)))
    count = levels // CHUNKS
    n = count * own
    flops = 6 * count * own * cells * coeffs
    nbytes = 4 * n * (cells + coeffs) + 4 * cells * coeffs
    factor = (coeffs // 2) / float(cells * cells)
    spread = jax.ShapeDtypeStruct((bands, rows, n), F32)

    def exchange(a):
        return lax.all_to_all(a, BAND, 0, 0, tiled=True)

    first = stage(
        functools.partial(synth_y, count, rows, bands),
        spread,
        [pltpu.VMEM((count * rows, coeffs), BF16)] * 2 + [pltpu.VMEM((count * rows, 256), F32)],
        flops, nbytes,
    )
    second = stage(
        synth_x,
        (jax.ShapeDtypeStruct((cells, n), F32), jax.ShapeDtypeStruct((bands, 8, LANES), F32)),
        [pltpu.VMEM((coeffs, n), BF16)] * 2,
        flops, nbytes,
    )
    third = stage(
        functools.partial(analyse_x, float(cells * cells)),
        spread,
        [pltpu.VMEM((cells, n), BF16)] * 2 + [pltpu.VMEM((coeffs, 256), F32)],
        flops, nbytes,
    )
    fourth = stage(
        functools.partial(analyse_y, count, factor),
        jax.ShapeDtypeStruct((count, rows, coeffs), F32),
        [pltpu.VMEM((count * rows, cells), BF16)] * 2,
        flops, nbytes,
    )
    done = []
    for k in range(CHUNKS):
        sent = first(spectral[k * count : (k + 1) * count], uh, ul)
        turned = exchange(sent)
        product, energy = second(turned, th, tl, coupling)
        energy = exchange(energy)
        back = third(product, energy, quadratic, uh, ul)
        done.append(fourth(exchange(back), th, tl))
    return jnp.concatenate(done, axis=0) if CHUNKS > 1 else done[0]


def solution(mesh):
    torus = Mesh(
        mesh.devices.reshape(mesh.shape["member"], 2, 4, 2),
        ("member",) + BAND,
    )
    return jax.shard_map(
        functools.partial(on_device, mesh.shape["band"]),
        mesh=torus,
        in_specs=(P("member", BAND, None), P(MEMBER_BAND, None), P(MEMBER_BAND, None)),
        out_specs=P("member", BAND, None),
        check_vma=False,
    )
```

```python
import functools, math
import numpy as np
import jax
import jax.numpy as jnp
from jax import lax
from jax.experimental import pallas as pl
from jax.experimental.pallas import tpu as pltpu
from jax.sharding import Mesh
from jax.sharding import PartitionSpec as P

F32, BF16 = jnp.float32, jnp.bfloat16
LANES = 128

BAND = ("band_0", "band_1", "band_2")
MEMBER_BAND = ("member",) + BAND


def trig_table(cells, coeffs):
    half = coeffs // 2
    position = np.arange(cells)[:, None]
    column = np.arange(coeffs)[None, :]
    turns = position * (column % half) % cells
    angles = turns * (2.0 * np.pi / cells)
    return np.where(column < half, np.cos(angles), np.sin(angles)).astype(np.float32)


def split_table(table):
    high = table.astype(jnp.bfloat16)
    low = (table - high.astype(np.float32)).astype(jnp.bfloat16)
    return high, low


def split(value):
    high = value.astype(BF16)
    return high, (value - high.astype(F32)).astype(BF16)


def dot(a, b):
    return jnp.dot(a, b, preferred_element_type=F32)


def dot3(a_high, a_low, b_high, b_low):
    return dot(a_high, b_high) + dot(a_low, b_high) + dot(a_high, b_low)


def lane_halves(shape):
    return lax.broadcasted_iota(jnp.int32, shape, 1) < LANES // 2


def swap(a, b):
    left = lane_halves(a.shape)
    return (
        jnp.where(left, a, pltpu.roll(b, LANES // 2, 1)),
        jnp.where(left, pltpu.roll(a, LANES // 2, 1), b),
    )


def synth_y(levels, rows, x_ref, th_ref, tl_ref, o_ref, xh, xl, acc):
    @pl.when(pl.program_id(0) == 0)
    def _():
        high, low = split(x_ref[...].reshape(levels * rows, x_ref.shape[2]))
        xh[...] = high
        xl[...] = low

    acc[...] = dot3(xh[...], xl[...], th_ref[...], tl_ref[...])
    for p in range(levels // 2):
        for h in range(2):
            a = acc[2 * p * rows : (2 * p + 1) * rows, h * LANES : (h + 1) * LANES]
            b = acc[(2 * p + 1) * rows : (2 * p + 2) * rows, h * LANES : (h + 1) * LANES]
            even, odd = swap(a, b)
            o_ref[2 * h, p] = even
            o_ref[2 * h + 1, p] = odd


def reversed_rows(block, fill):
    count = block.shape[0]
    row = lax.broadcasted_iota(jnp.int32, (count, count), 0)
    col = lax.broadcasted_iota(jnp.int32, (count, count), 1)
    flip = jnp.where(row + col == count, 1.0, 0.0).astype(BF16)
    high = block.astype(BF16)
    rest = block - high.astype(F32)
    middle = rest.astype(BF16)
    low = (rest - middle.astype(F32)).astype(BF16)
    turned = dot(flip, high) + dot(flip, middle) + dot(flip, low)
    return first_row(turned, fill)


def first_row(block, fill):
    row = lax.broadcasted_iota(jnp.int32, block.shape, 0)
    return jnp.where(row == 0, fill, block)


def folded_field(a, out):
    turned = jnp.concatenate([a, a], axis=0).T
    q = turned.shape[0] // 4
    out[0:q] = turned[0:q]
    out[q : 2 * q] = reversed_rows(turned[q : 2 * q], turned[2 * q : 2 * q + 1])
    out[2 * q : 3 * q] = reversed_rows(turned[3 * q :], turned[q : q + 1])
    out[3 * q :] = first_row(turned[2 * q : 3 * q], turned[3 * q : 3 * q + 1])


def alternate(count):
    row = lax.broadcasted_iota(jnp.int32, (count, 1), 0)
    return jnp.where(row % 2 == 0, 1.0, -1.0).astype(F32)


SUB = 64


def synth_x(r_ref, th_ref, tl_ref, c_ref, p_ref, e_ref, rh, rl, basis, field):
    bands, groups, rows, _ = r_ref.shape
    n = groups * LANES
    few = rows // 2
    quarter = th_ref.shape[1]
    folded_field(c_ref[...] * (1.0 / (bands * rows // 2)), field)
    corner = {f: [jnp.zeros((1, LANES), F32)] * groups for f in (0, 3)}
    for f in range(4):
        for i in range(bands // 4):
            s = (f // 2) * (bands // 2) + 2 * i
            for g in range(groups):
                lanes = slice(g * LANES, (g + 1) * LANES)
                part = jnp.concatenate([r_ref[s + t, g, pl.ds(f % 2, few, 2), :] for t in range(2)], axis=0)
                if f in corner:
                    corner[f][g] += jnp.sum(part * alternate(rows), axis=0, keepdims=True)
                high, low = split(part)
                rh[f, i * rows : (i + 1) * rows, lanes] = high
                rl[f, i * rows : (i + 1) * rows, lanes] = low
    e_ref[...] = jnp.zeros_like(e_ref)
    for j in range(n // 256):
        cols = slice(j * 256, (j + 1) * 256)
        for f in range(4):
            basis[f] = dot3(th_ref[f], tl_ref[f], rh[f, :, cols], rl[f, :, cols])
        for h in range(2):
            lanes = slice(h * LANES, (h + 1) * LANES)
            target = slice(j * 256 + h * LANES, j * 256 + (h + 1) * LANES)
            total = jnp.zeros((1, LANES), F32)
            for r in range(0, quarter, SUB):
                ce, co, se, so = (basis[f, r : r + SUB, lanes] for f in range(4))
                plus, minus, both, less = ce + co, ce - co, se + so, so - se
                blocks = [plus + both, minus + less, plus - both, minus - less]
                if r == 0:
                    blocks[2] = first_row(blocks[2], corner[0][2 * j + h] + corner[3][2 * j + h])
                    blocks[3] = first_row(blocks[3], corner[0][2 * j + h] - corner[3][2 * j + h])
                for b, block in enumerate(blocks):
                    at = slice(b * quarter + r, b * quarter + r + SUB)
                    product = block * field[at, :]
                    p_ref[at, target] = product
                    total += jnp.sum(product * product, axis=0, keepdims=True)
            for d in range(e_ref.shape[0]):
                e_ref[d, 2 * j + h : 2 * j + h + 1, :] = total


def group_sum(v):
    lane = lax.broadcasted_iota(jnp.int32, v.shape, 1)
    step = 1
    while step < LANES // 2:
        v = v + jnp.where(lane % (2 * step) < step, pltpu.roll(v, LANES - step, 1), pltpu.roll(v, step, 1))
        step *= 2
    return v


def analyse_x(points, p_ref, e_ref, q_ref, th_ref, tl_ref, o_ref, gh, gl, corners, field):
    bands, groups, rows, _ = o_ref.shape
    n = groups * LANES
    few = rows // 2
    coeffs, quarter = th_ref.shape[1], th_ref.shape[2]
    folded_field(q_ref[...], field)
    total = group_sum(jnp.sum(e_ref[...], axis=0))
    scale = lax.rsqrt(total * (1.0 / points) + 1e-06)
    for t in range(n // LANES):
        lanes = slice(t * LANES, (t + 1) * LANES)
        for r in range(0, quarter, SUB):
            g = []
            for b in range(4):
                at = slice(b * quarter + r, b * quarter + r + SUB)
                scaled = p_ref[at, lanes] * scale[t : t + 1, :]
                g.append(scaled + field[at, :] * scaled * scaled)
            sum0, less0, sum1, less1 = g[0] + g[1], g[0] - g[1], g[2] + g[3], g[2] - g[3]
            folded = [sum0 + sum1, less0 + less1, less0 - less1, sum0 - sum1]
            if r == 0:
                corners[0:1, lanes] = sum1[0:1]
                corners[1:2, lanes] = less1[0:1]
                folded[0] = first_row(folded[0], sum0[0:1])
                folded[1] = first_row(folded[1], less0[0:1])
            for f in range(4):
                high, low = split(folded[f])
                gh[f, r : r + SUB, lanes] = high
                gl[f, r : r + SUB, lanes] = low
    row = lax.broadcasted_iota(jnp.int32, (coeffs, 1), 0)
    for j in range(n // 256):
        cols = slice(j * 256, (j + 1) * 256)
        for f in range(4):
            value = dot3(th_ref[f], tl_ref[f], gh[f, :, cols], gl[f, :, cols])
            if f in (0, 3):
                value += alternate(coeffs) * corners[f // 3 : f // 3 + 1, cols]
            value *= jnp.where(row == 0, 1.0 if f == 0 else 2.0, 2.0).astype(F32)
            for i in range(bands // 2):
                for h in range(2):
                    o_ref[(f // 2) * (bands // 2) + i, 2 * j + h, pl.ds(f % 2, few, 2), :] = value[
                        i * few : (i + 1) * few, h * LANES : (h + 1) * LANES
                    ]


def analyse_y(levels, factor, r_ref, th_ref, tl_ref, o_ref, yh, yl):
    bands, rows = r_ref.shape[0], r_ref.shape[2]
    for p in range(levels // 2):
        for s in range(bands // 2):
            a = r_ref[2 * s, p]
            b = r_ref[2 * s + 1, p]
            for i, piece in enumerate(swap(a, b)):
                high, low = split(piece)
                at = (2 * p + i) * rows
                yh[at : at + rows, s * LANES : (s + 1) * LANES] = high
                yl[at : at + rows, s * LANES : (s + 1) * LANES] = low
    coeffs = th_ref.shape[1]
    for j in range(coeffs // 256):
        cols = slice(j * 256, (j + 1) * 256)
        col = j * 256 + lax.broadcasted_iota(jnp.int32, (1, 256), 1)
        weight = jnp.where(col % (coeffs // 2) == 0, factor, 2.0 * factor).astype(F32)
        value = dot3(yh[...], yl[...], th_ref[:, cols], tl_ref[:, cols]) * weight
        o_ref[:, :, cols] = value.reshape(levels, rows, 256)


def stage(kernel, in_specs, out_shape, scratch, flops, nbytes, limit=16):
    return pl.pallas_call(
        kernel,
        in_specs=[pl.BlockSpec(memory_space=m) for m in in_specs],
        out_shape=out_shape,
        scratch_shapes=scratch,
        compiler_params=pltpu.CompilerParams(vmem_limit_bytes=limit * 1024 * 1024),
        cost_estimate=pl.CostEstimate(flops=flops, bytes_accessed=nbytes, transcendentals=0),
    )


def on_device(bands, spectral, coupling, quadratic):
    levels, rows, coeffs = spectral.shape
    own, cells = coupling.shape
    quarter = cells // 4
    table = trig_table(cells, coeffs)
    th, tl = (jnp.asarray(t) for t in split_table(table))
    yh, yl = (jnp.asarray(np.stack(np.split(t, 4, 1))) for t in split_table(np.ascontiguousarray(table.T)))
    folds = np.stack([table[:quarter, f // 2 * (coeffs // 2) + f % 2 :: 2][:, : coeffs // 4] for f in range(4)])
    fh, fl = (jnp.asarray(t) for t in split_table(folds))
    bh, bl = (jnp.asarray(t) for t in split_table(np.ascontiguousarray(folds.transpose(0, 2, 1))))
    n = levels * own
    flops = 6 * n * cells * coeffs
    nbytes = 4 * n * (cells + coeffs) + 4 * cells * coeffs
    factor = (coeffs // 2) / float(cells * cells)
    spread = jax.ShapeDtypeStruct((bands, n // LANES, rows, LANES), F32)
    vmem = pltpu.VMEM

    def exchange(a):
        return lax.all_to_all(a, BAND, 0, 0, tiled=True)

    first = pl.pallas_call(
        functools.partial(synth_y, levels, rows),
        grid=(bands // 4,),
        in_specs=[
            pl.BlockSpec((levels, rows, coeffs), lambda j: (0, 0, 0)),
            pl.BlockSpec((None, coeffs, 256), lambda j: (j, 0, 0)),
            pl.BlockSpec((None, coeffs, 256), lambda j: (j, 0, 0)),
        ],
        out_specs=pl.BlockSpec((4, n // LANES, rows, LANES), lambda j: (j, 0, 0, 0)),
        out_shape=spread,
        scratch_shapes=[vmem((levels * rows, coeffs), BF16)] * 2 + [vmem((levels * rows, 256), F32)],
        compiler_params=pltpu.CompilerParams(vmem_limit_bytes=60 * 1024 * 1024),
        cost_estimate=pl.CostEstimate(flops=flops, bytes_accessed=nbytes, transcendentals=0),
    )
    second = stage(
        synth_x, [vmem] * 4,
        (jax.ShapeDtypeStruct((cells, n), F32), jax.ShapeDtypeStruct((bands, 8, LANES), F32)),
        [vmem((4, coeffs // 4, n), BF16)] * 2 + [vmem((4, quarter, 256), F32), vmem((cells, LANES), F32)],
        flops, nbytes,
    )
    third = stage(
        functools.partial(analyse_x, float(cells * cells)), [vmem] * 5, spread,
        [vmem((4, quarter, n), BF16)] * 2 + [vmem((8, n), F32), vmem((cells, LANES), F32)],
        flops, nbytes,
    )
    fourth = stage(
        functools.partial(analyse_y, levels, factor), [vmem] * 3,
        jax.ShapeDtypeStruct((levels, rows, coeffs), F32),
        [vmem((levels * rows, cells), BF16)] * 2,
        flops, nbytes,
    )
    turned = exchange(first(spectral, yh, yl))
    product, energy = second(turned, fh, fl, coupling)
    back = exchange(third(product, exchange(energy), quadratic, bh, bl))
    return fourth(back, th, tl)


def solution(mesh):
    torus = Mesh(
        mesh.devices.reshape(mesh.shape["member"], 2, 4, 2),
        ("member",) + BAND,
    )
    return jax.shard_map(
        functools.partial(on_device, mesh.shape["band"]),
        mesh=torus,
        in_specs=(P("member", BAND, None), P(MEMBER_BAND, None), P(MEMBER_BAND, None)),
        out_specs=P("member", BAND, None),
        check_vma=False,
    )
```

```python
import functools, math
import numpy as np
import jax
import jax.numpy as jnp
from jax import lax
from jax.experimental import pallas as pl
from jax.experimental.pallas import tpu as pltpu
from jax.sharding import Mesh
from jax.sharding import PartitionSpec as P

F32, BF16 = jnp.float32, jnp.bfloat16
LANES = 128

BAND = ("band_0", "band_1", "band_2")
MEMBER_BAND = ("member",) + BAND


def trig_table(cells, coeffs):
    half = coeffs // 2
    position = np.arange(cells)[:, None]
    column = np.arange(coeffs)[None, :]
    turns = position * (column % half) % cells
    angles = turns * (2.0 * np.pi / cells)
    return np.where(column < half, np.cos(angles), np.sin(angles)).astype(np.float32)


def split_table(table):
    high = table.astype(jnp.bfloat16)
    low = (table - high.astype(np.float32)).astype(jnp.bfloat16)
    return high, low


def split(value):
    high = value.astype(BF16)
    return high, (value - high.astype(F32)).astype(BF16)


def dot(a, b):
    return jnp.dot(a, b, preferred_element_type=F32)


def dot3(a_high, a_low, b_high, b_low):
    return dot(a_high, b_high) + dot(a_low, b_high) + dot(a_high, b_low)


def lane_halves(shape):
    return lax.broadcasted_iota(jnp.int32, shape, 1) < LANES // 2


def swap(a, b):
    left = lane_halves(a.shape)
    return (
        jnp.where(left, a, pltpu.roll(b, LANES // 2, 1)),
        jnp.where(left, pltpu.roll(a, LANES // 2, 1), b),
    )


def synth_y(levels, rows, x_ref, th_ref, tl_ref, o_ref, xh, xl, acc):
    @pl.when(pl.program_id(0) == 0)
    def _():
        high, low = split(x_ref[...].reshape(levels * rows, x_ref.shape[2]))
        xh[...] = high
        xl[...] = low

    acc[...] = dot3(xh[...], xl[...], th_ref[...], tl_ref[...])
    for p in range(levels // 2):
        for h in range(2):
            a = acc[2 * p * rows : (2 * p + 1) * rows, h * LANES : (h + 1) * LANES]
            b = acc[(2 * p + 1) * rows : (2 * p + 2) * rows, h * LANES : (h + 1) * LANES]
            even, odd = swap(a, b)
            o_ref[2 * h, p] = even
            o_ref[2 * h + 1, p] = odd


def picked(choice, value):
    choice = jnp.where(choice, 1.0, 0.0).astype(BF16)
    high = value.astype(BF16)
    rest = value - high.astype(F32)
    middle = rest.astype(BF16)
    low = (rest - middle.astype(F32)).astype(BF16)
    return dot(choice, high) + dot(choice, middle) + dot(choice, low)


def positions(count):
    return tuple(lax.broadcasted_iota(jnp.int32, (count, count), d) for d in range(2))


def reversed_rows(block, fill):
    count = block.shape[0]
    row, col = positions(count)
    return first_row(picked(row + col == count, block), fill)


def band_order(a):
    count = a.shape[0]
    row, col = positions(count)
    upper = lax.axis_index(BAND[0])
    return picked(col == row + upper * (count - 1 - 2 * row), a)


def first_row(block, fill):
    row = lax.broadcasted_iota(jnp.int32, block.shape, 0)
    return jnp.where(row == 0, fill, block)


def folded_field(a, out):
    a = band_order(a)
    turned = jnp.concatenate([a, a], axis=0).T
    q = turned.shape[0] // 4
    out[0:q] = turned[0:q]
    out[q : 2 * q] = reversed_rows(turned[q : 2 * q], turned[2 * q : 2 * q + 1])
    out[2 * q : 3 * q] = reversed_rows(turned[3 * q :], turned[q : q + 1])
    out[3 * q :] = first_row(turned[2 * q : 3 * q], turned[3 * q : 3 * q + 1])


def alternate(count):
    row = lax.broadcasted_iota(jnp.int32, (count, 1), 0)
    return jnp.where(row % 2 == 0, 1.0, -1.0).astype(F32)


SUB = 64
PIECES = 4


def synth_x(r_ref, th_ref, tl_ref, c_ref, p_ref, e_ref, rh, rl, basis, field):
    bands, groups, rows, _ = r_ref.shape
    n = groups * LANES
    few = rows // 2
    quarter = th_ref.shape[1]
    folded_field(c_ref[...] * (1.0 / (bands * rows // 2)), field)
    corner = {f: [jnp.zeros((1, LANES), F32)] * groups for f in (0, 3)}
    for f in range(4):
        for i in range(bands // 4):
            s = (f // 2) * (bands // 2) + 2 * i
            for g in range(groups):
                lanes = slice(g * LANES, (g + 1) * LANES)
                part = jnp.concatenate([r_ref[s + t, g, pl.ds(f % 2, few, 2), :] for t in range(2)], axis=0)
                if f in corner:
                    corner[f][g] += jnp.sum(part * alternate(rows), axis=0, keepdims=True)
                high, low = split(part)
                rh[f, i * rows : (i + 1) * rows, lanes] = high
                rl[f, i * rows : (i + 1) * rows, lanes] = low
    e_ref[...] = jnp.zeros_like(e_ref)
    for j in range(n // 256):
        cols = slice(j * 256, (j + 1) * 256)
        for f in range(4):
            basis[f] = dot3(th_ref[f], tl_ref[f], rh[f, :, cols], rl[f, :, cols])
        for h in range(2):
            lanes = slice(h * LANES, (h + 1) * LANES)
            target = slice(j * 256 + h * LANES, j * 256 + (h + 1) * LANES)
            total = jnp.zeros((1, LANES), F32)
            for r in range(0, quarter, SUB):
                ce, co, se, so = (basis[f, r : r + SUB, lanes] for f in range(4))
                plus, minus, both, less = ce + co, ce - co, se + so, so - se
                blocks = [plus + both, minus + less, plus - both, minus - less]
                if r == 0:
                    blocks[2] = first_row(blocks[2], corner[0][2 * j + h] + corner[3][2 * j + h])
                    blocks[3] = first_row(blocks[3], corner[0][2 * j + h] - corner[3][2 * j + h])
                for b, block in enumerate(blocks):
                    at = slice(b * quarter + r, b * quarter + r + SUB)
                    product = block * field[at, :]
                    p_ref[at, target] = product
                    total += jnp.sum(product * product, axis=0, keepdims=True)
            for d in range(e_ref.shape[0]):
                e_ref[d, 2 * j + h : 2 * j + h + 1, :] = total


def group_sum(v):
    lane = lax.broadcasted_iota(jnp.int32, v.shape, 1)
    step = 1
    while step < LANES // 2:
        v = v + jnp.where(lane % (2 * step) < step, pltpu.roll(v, LANES - step, 1), pltpu.roll(v, step, 1))
        step *= 2
    return v


def analyse_x(points, p_ref, e_ref, q_ref, th_ref, tl_ref, o_ref, gh, gl, corners, field):
    bands, groups, rows, _ = o_ref.shape
    n = groups * LANES
    few = rows // 2
    coeffs, quarter = th_ref.shape[1], th_ref.shape[2]
    folded_field(q_ref[...], field)
    total = group_sum(jnp.sum(e_ref[...], axis=0))
    scale = lax.rsqrt(total * (1.0 / points) + 1e-06)
    for t in range(n // LANES):
        lanes = slice(t * LANES, (t + 1) * LANES)
        for r in range(0, quarter, SUB):
            g = []
            for b in range(4):
                at = slice(b * quarter + r, b * quarter + r + SUB)
                scaled = p_ref[at, lanes] * scale[t : t + 1, :]
                g.append(scaled + field[at, :] * scaled * scaled)
            sum0, less0, sum1, less1 = g[0] + g[1], g[0] - g[1], g[2] + g[3], g[2] - g[3]
            folded = [sum0 + sum1, less0 + less1, less0 - less1, sum0 - sum1]
            if r == 0:
                corners[0:1, lanes] = sum1[0:1]
                corners[1:2, lanes] = less1[0:1]
                folded[0] = first_row(folded[0], sum0[0:1])
                folded[1] = first_row(folded[1], less0[0:1])
            for f in range(4):
                high, low = split(folded[f])
                gh[f, r : r + SUB, lanes] = high
                gl[f, r : r + SUB, lanes] = low
    row = lax.broadcasted_iota(jnp.int32, (coeffs, 1), 0)
    for j in range(n // 256):
        cols = slice(j * 256, (j + 1) * 256)
        for f in range(4):
            value = dot3(th_ref[f], tl_ref[f], gh[f, :, cols], gl[f, :, cols])
            if f in (0, 3):
                value += alternate(coeffs) * corners[f // 3 : f // 3 + 1, cols]
            value *= jnp.where(row == 0, 1.0 if f == 0 else 2.0, 2.0).astype(F32)
            for i in range(bands // 2):
                for h in range(2):
                    o_ref[(f // 2) * (bands // 2) + i, 2 * j + h, pl.ds(f % 2, few, 2), :] = value[
                        i * few : (i + 1) * few, h * LANES : (h + 1) * LANES
                    ]


def analyse_y(levels, factor, r_ref, th_ref, tl_ref, o_hbm, yh, yl, edge, o_ref, sem):
    bands, rows = r_ref.shape[0], r_ref.shape[2]
    half = th_ref.shape[2]
    start = lax.broadcasted_iota(jnp.int32, (rows, LANES), 1) == 0
    col = lax.broadcasted_iota(jnp.int32, (1, half), 1)
    weight = jnp.where(col == 0, factor, 2.0 * factor).astype(F32)
    pieces = sem.shape[0]
    step = levels // pieces
    copies = []
    for g in range(pieces):
        for p in range(g * step // 2, (g + 1) * step // 2):
            before = [jnp.zeros((rows, LANES), F32)] * 2
            for s in range(bands // 4):
                lower = swap(r_ref[2 * s, p], r_ref[2 * s + 1, p])
                upper = swap(r_ref[bands - 1 - 2 * s, p], r_ref[bands - 2 - 2 * s, p])
                for i in range(2):
                    at = slice((2 * p + i) * rows, (2 * p + i + 1) * rows)
                    shifted = pltpu.roll(upper[i], 1, 1)
                    mirror = jnp.where(start, before[i], shifted)
                    before[i] = shifted
                    for f, value in enumerate((lower[i] + mirror, lower[i] - mirror)):
                        high, low = split(value)
                        yh[f, at, s * LANES : (s + 1) * LANES] = high
                        yl[f, at, s * LANES : (s + 1) * LANES] = low
            for i in range(2):
                edge[(2 * p + i) * rows : (2 * p + i + 1) * rows, :] = before[i]
        at = slice(g * step * rows, (g + 1) * step * rows)
        for f in range(2):
            value = dot3(yh[f, at], yl[f, at], th_ref[f], tl_ref[f])
            if f == 0:
                value += edge[at, 0:1] * jnp.where(col % 2 == 0, 1.0, -1.0).astype(F32)
            o_ref[g * step : (g + 1) * step, :, f * half : (f + 1) * half] = (value * weight).reshape(step, rows, half)
        part = pl.ds(g * step, step)
        copies.append(pltpu.make_async_copy(o_ref.at[part], o_hbm.at[part], sem.at[g]))
        copies[-1].start()
    for copy in copies:
        copy.wait()


def stage(kernel, in_specs, out_shape, scratch, flops, nbytes, out_specs=None):
    return pl.pallas_call(
        kernel,
        in_specs=[pl.BlockSpec(memory_space=m) for m in in_specs],
        **({} if out_specs is None else {"out_specs": out_specs}),
        out_shape=out_shape,
        scratch_shapes=scratch,
        compiler_params=pltpu.CompilerParams(vmem_limit_bytes=16 * 1024 * 1024),
        cost_estimate=pl.CostEstimate(flops=flops, bytes_accessed=nbytes, transcendentals=0),
    )


def on_device(bands, spectral, coupling, quadratic):
    levels, rows, coeffs = spectral.shape
    own, cells = coupling.shape
    quarter = cells // 4
    table = trig_table(cells, coeffs)
    halves = np.stack([table[: cells // 2, : coeffs // 2], table[: cells // 2, coeffs // 2 :]])
    th, tl = (jnp.asarray(t) for t in split_table(halves))
    order = np.arange(cells).reshape(bands, own)
    order[bands // 2 :] = order[bands // 2 :, ::-1]
    ordered = np.ascontiguousarray(table[order.reshape(-1)].T)
    yh, yl = (jnp.asarray(np.stack(np.split(t, 4, 1))) for t in split_table(ordered))
    folds = np.stack([table[:quarter, f // 2 * (coeffs // 2) + f % 2 :: 2][:, : coeffs // 4] for f in range(4)])
    fh, fl = (jnp.asarray(t) for t in split_table(folds))
    bh, bl = (jnp.asarray(t) for t in split_table(np.ascontiguousarray(folds.transpose(0, 2, 1))))
    n = levels * own
    flops = 6 * n * cells * coeffs
    nbytes = 4 * n * (cells + coeffs) + 4 * cells * coeffs
    factor = (coeffs // 2) / float(cells * cells)
    spread = jax.ShapeDtypeStruct((bands, n // LANES, rows, LANES), F32)
    vmem = pltpu.VMEM

    def exchange(a):
        return lax.all_to_all(a, BAND, 0, 0, tiled=True)

    first = pl.pallas_call(
        functools.partial(synth_y, levels, rows),
        grid=(bands // 4,),
        in_specs=[
            pl.BlockSpec((levels, rows, coeffs), lambda j: (0, 0, 0)),
            pl.BlockSpec((None, coeffs, 256), lambda j: (j, 0, 0)),
            pl.BlockSpec((None, coeffs, 256), lambda j: (j, 0, 0)),
        ],
        out_specs=pl.BlockSpec((4, n // LANES, rows, LANES), lambda j: (j, 0, 0, 0)),
        out_shape=spread,
        scratch_shapes=[vmem((levels * rows, coeffs), BF16)] * 2 + [vmem((levels * rows, 256), F32)],
        compiler_params=pltpu.CompilerParams(vmem_limit_bytes=60 * 1024 * 1024),
        cost_estimate=pl.CostEstimate(flops=flops, bytes_accessed=nbytes, transcendentals=0),
    )
    second = stage(
        synth_x, [vmem] * 4,
        (jax.ShapeDtypeStruct((cells, n), F32), jax.ShapeDtypeStruct((bands, 8, LANES), F32)),
        [vmem((4, coeffs // 4, n), BF16)] * 2 + [vmem((4, quarter, 256), F32), vmem((cells, LANES), F32)],
        flops, nbytes,
    )
    third = stage(
        functools.partial(analyse_x, float(cells * cells)), [vmem] * 5, spread,
        [vmem((4, quarter, n), BF16)] * 2 + [vmem((8, n), F32), vmem((cells, LANES), F32)],
        flops, nbytes,
    )
    fourth = stage(
        functools.partial(analyse_y, levels, factor), [vmem] * 3,
        jax.ShapeDtypeStruct((levels, rows, coeffs), F32),
        [vmem((2, levels * rows, cells // 2), BF16)] * 2 + [
            vmem((levels * rows, LANES), F32), vmem((levels, rows, coeffs), F32), pltpu.SemaphoreType.DMA((PIECES,))
        ],
        flops, nbytes, pl.BlockSpec(memory_space=pl.ANY),
    )
    turned = exchange(first(spectral, yh, yl))
    product, energy = second(turned, fh, fl, coupling)
    back = exchange(third(product, exchange(energy), quadratic, bh, bl))
    return fourth(back, th, tl)


def solution(mesh):
    torus = Mesh(
        mesh.devices.reshape(mesh.shape["member"], 2, 4, 2),
        ("member",) + BAND,
    )
    return jax.shard_map(
        functools.partial(on_device, mesh.shape["band"]),
        mesh=torus,
        in_specs=(P("member", BAND, None), P(MEMBER_BAND, None), P(MEMBER_BAND, None)),
        out_specs=P("member", BAND, None),
        check_vma=False,
    )
```

```python
import functools, math
import numpy as np
import jax
import jax.numpy as jnp
from jax import lax
from jax.experimental import pallas as pl
from jax.experimental.pallas import tpu as pltpu
from jax.sharding import Mesh
from jax.sharding import PartitionSpec as P

F32, BF16 = jnp.float32, jnp.bfloat16
LANES = 128

BAND = ("band_0", "band_1", "band_2")
MEMBER_BAND = ("member",) + BAND


def trig_table(cells, coeffs):
    half = coeffs // 2
    position = np.arange(cells)[:, None]
    column = np.arange(coeffs)[None, :]
    turns = position * (column % half) % cells
    angles = turns * (2.0 * np.pi / cells)
    return np.where(column < half, np.cos(angles), np.sin(angles)).astype(np.float32)


def split_table(table):
    high = table.astype(jnp.bfloat16)
    low = (table - high.astype(np.float32)).astype(jnp.bfloat16)
    return high, low


def split(value):
    high = value.astype(BF16)
    return high, (value - high.astype(F32)).astype(BF16)


def dot(a, b):
    return jnp.dot(a, b, preferred_element_type=F32)


def dot3(a_high, a_low, b_high, b_low):
    return dot(a_high, b_high) + dot(a_low, b_high) + dot(a_high, b_low)


def lane_halves(shape):
    return lax.broadcasted_iota(jnp.int32, shape, 1) < LANES // 2


def swap(a, b):
    left = lane_halves(a.shape)
    return (
        jnp.where(left, a, pltpu.roll(b, LANES // 2, 1)),
        jnp.where(left, pltpu.roll(a, LANES // 2, 1), b),
    )


def synth_y(levels, rows, x_ref, th_ref, tl_ref, o_ref, xh, xl, acc):
    @pl.when(pl.program_id(0) == 0)
    def _():
        high, low = split(x_ref[...].reshape(levels * rows, x_ref.shape[2]))
        xh[...] = high
        xl[...] = low

    acc[...] = dot3(xh[...], xl[...], th_ref[...], tl_ref[...])
    for p in range(levels // 2):
        for h in range(2):
            a = acc[2 * p * rows : (2 * p + 1) * rows, h * LANES : (h + 1) * LANES]
            b = acc[(2 * p + 1) * rows : (2 * p + 2) * rows, h * LANES : (h + 1) * LANES]
            even, odd = swap(a, b)
            o_ref[2 * h, p] = even
            o_ref[2 * h + 1, p] = odd


def picked(choice, value):
    choice = jnp.where(choice, 1.0, 0.0).astype(BF16)
    high = value.astype(BF16)
    rest = value - high.astype(F32)
    middle = rest.astype(BF16)
    low = (rest - middle.astype(F32)).astype(BF16)
    return dot(choice, high) + dot(choice, middle) + dot(choice, low)


def positions(count):
    return tuple(lax.broadcasted_iota(jnp.int32, (count, count), d) for d in range(2))


def reversed_rows(block, fill):
    count = block.shape[0]
    row, col = positions(count)
    return first_row(picked(row + col == count, block), fill)


def band_order(a):
    count = a.shape[0]
    row, col = positions(count)
    upper = lax.axis_index(BAND[0])
    return picked(col == row + upper * (count - 1 - 2 * row), a)


def first_row(block, fill):
    row = lax.broadcasted_iota(jnp.int32, block.shape, 0)
    return jnp.where(row == 0, fill, block)


def folded_field(a, out):
    a = band_order(a)
    turned = jnp.concatenate([a, a], axis=0).T
    q = turned.shape[0] // 4
    out[0:q] = turned[0:q]
    out[q : 2 * q] = reversed_rows(turned[q : 2 * q], turned[2 * q : 2 * q + 1])
    out[2 * q : 3 * q] = reversed_rows(turned[3 * q :], turned[q : q + 1])
    out[3 * q :] = first_row(turned[2 * q : 3 * q], turned[3 * q : 3 * q + 1])


def alternate(count):
    row = lax.broadcasted_iota(jnp.int32, (count, 1), 0)
    return jnp.where(row % 2 == 0, 1.0, -1.0).astype(F32)


SUB = 64
PIECES = 8


def synth_x(r_ref, th_ref, tl_ref, c_ref, p_ref, e_ref, rh, rl, basis, field):
    bands, groups, rows, _ = r_ref.shape
    n = groups * LANES
    few = rows // 2
    quarter = th_ref.shape[1]
    folded_field(c_ref[...] * (1.0 / (bands * rows // 2)), field)
    corner = {f: [jnp.zeros((1, LANES), F32)] * groups for f in (0, 3)}
    for f in range(4):
        for i in range(bands // 4):
            s = (f // 2) * (bands // 2) + 2 * i
            for g in range(groups):
                lanes = slice(g * LANES, (g + 1) * LANES)
                part = jnp.concatenate([r_ref[s + t, g, pl.ds(f % 2, few, 2), :] for t in range(2)], axis=0)
                if f in corner:
                    corner[f][g] += jnp.sum(part * alternate(rows), axis=0, keepdims=True)
                high, low = split(part)
                rh[f, i * rows : (i + 1) * rows, lanes] = high
                rl[f, i * rows : (i + 1) * rows, lanes] = low
    e_ref[...] = jnp.zeros_like(e_ref)
    for j in range(n // 256):
        cols = slice(j * 256, (j + 1) * 256)
        for f in range(4):
            basis[f] = dot3(th_ref[f], tl_ref[f], rh[f, :, cols], rl[f, :, cols])
        for h in range(2):
            lanes = slice(h * LANES, (h + 1) * LANES)
            target = slice(j * 256 + h * LANES, j * 256 + (h + 1) * LANES)
            total = jnp.zeros((1, LANES), F32)
            for r in range(0, quarter, SUB):
                ce, co, se, so = (basis[f, r : r + SUB, lanes] for f in range(4))
                plus, minus, both, less = ce + co, ce - co, se + so, so - se
                blocks = [plus + both, minus + less, plus - both, minus - less]
                if r == 0:
                    blocks[2] = first_row(blocks[2], corner[0][2 * j + h] + corner[3][2 * j + h])
                    blocks[3] = first_row(blocks[3], corner[0][2 * j + h] - corner[3][2 * j + h])
                for b, block in enumerate(blocks):
                    at = slice(b * quarter + r, b * quarter + r + SUB)
                    product = block * field[at, :]
                    p_ref[at, target] = product
                    total += jnp.sum(product * product, axis=0, keepdims=True)
            for d in range(e_ref.shape[0]):
                e_ref[d, 2 * j + h : 2 * j + h + 1, :] = total


def group_sum(v):
    lane = lax.broadcasted_iota(jnp.int32, v.shape, 1)
    step = 1
    while step < LANES // 2:
        v = v + jnp.where(lane % (2 * step) < step, pltpu.roll(v, LANES - step, 1), pltpu.roll(v, step, 1))
        step *= 2
    return v


def analyse_x(points, p_ref, e_ref, q_ref, th_ref, tl_ref, o_ref, gh, gl, corners, field):
    bands, groups, rows, _ = o_ref.shape
    n = groups * LANES
    few = rows // 2
    coeffs, quarter = th_ref.shape[1], th_ref.shape[2]
    folded_field(q_ref[...], field)
    total = group_sum(jnp.sum(e_ref[...], axis=0))
    scale = lax.rsqrt(total * (1.0 / points) + 1e-06)
    for t in range(n // LANES):
        lanes = slice(t * LANES, (t + 1) * LANES)
        for r in range(0, quarter, SUB):
            g = []
            for b in range(4):
                at = slice(b * quarter + r, b * quarter + r + SUB)
                scaled = p_ref[at, lanes] * scale[t : t + 1, :]
                g.append(scaled + field[at, :] * scaled * scaled)
            sum0, less0, sum1, less1 = g[0] + g[1], g[0] - g[1], g[2] + g[3], g[2] - g[3]
            folded = [sum0 + sum1, less0 + less1, less0 - less1, sum0 - sum1]
            if r == 0:
                corners[0:1, lanes] = sum1[0:1]
                corners[1:2, lanes] = less1[0:1]
                folded[0] = first_row(folded[0], sum0[0:1])
                folded[1] = first_row(folded[1], less0[0:1])
            for f in range(4):
                high, low = split(folded[f])
                gh[f, r : r + SUB, lanes] = high
                gl[f, r : r + SUB, lanes] = low
    row = lax.broadcasted_iota(jnp.int32, (coeffs, 1), 0)
    for j in range(n // 256):
        cols = slice(j * 256, (j + 1) * 256)
        for f in range(4):
            value = dot3(th_ref[f], tl_ref[f], gh[f, :, cols], gl[f, :, cols])
            if f in (0, 3):
                value += alternate(coeffs) * corners[f // 3 : f // 3 + 1, cols]
            value *= jnp.where(row == 0, 1.0 if f == 0 else 2.0, 2.0).astype(F32)
            for i in range(bands // 2):
                for h in range(2):
                    o_ref[(f // 2) * (bands // 2) + i, 2 * j + h, pl.ds(f % 2, few, 2), :] = value[
                        i * few : (i + 1) * few, h * LANES : (h + 1) * LANES
                    ]


def analyse_y(levels, factor, r_ref, th_ref, tl_ref, o_hbm, yh, yl, edge, o_ref, sem):
    bands, rows = r_ref.shape[0], r_ref.shape[2]
    half = th_ref.shape[2]
    start = lax.broadcasted_iota(jnp.int32, (rows, LANES), 1) == 0
    col = lax.broadcasted_iota(jnp.int32, (1, half), 1)
    weight = jnp.where(col == 0, factor, 2.0 * factor).astype(F32)
    pieces = sem.shape[0]
    step = levels // pieces
    copies = []
    for g in range(pieces):
        for p in range(g * step // 2, (g + 1) * step // 2):
            before = [jnp.zeros((rows, LANES), F32)] * 2
            for s in range(bands // 4):
                lower = swap(r_ref[2 * s, p], r_ref[2 * s + 1, p])
                upper = swap(r_ref[bands - 1 - 2 * s, p], r_ref[bands - 2 - 2 * s, p])
                for i in range(2):
                    at = slice((2 * p + i) * rows, (2 * p + i + 1) * rows)
                    shifted = pltpu.roll(upper[i], 1, 1)
                    mirror = jnp.where(start, before[i], shifted)
                    before[i] = shifted
                    for f, value in enumerate((lower[i] + mirror, lower[i] - mirror)):
                        high, low = split(value)
                        yh[f, at, s * LANES : (s + 1) * LANES] = high
                        yl[f, at, s * LANES : (s + 1) * LANES] = low
            for i in range(2):
                edge[(2 * p + i) * rows : (2 * p + i + 1) * rows, :] = before[i]
        at = slice(g * step * rows, (g + 1) * step * rows)
        for f in range(2):
            value = dot3(yh[f, at], yl[f, at], th_ref[f], tl_ref[f])
            if f == 0:
                value += edge[at, 0:1] * jnp.where(col % 2 == 0, 1.0, -1.0).astype(F32)
            o_ref[g * step : (g + 1) * step, :, f * half : (f + 1) * half] = (value * weight).reshape(step, rows, half)
        part = pl.ds(g * step, step)
        copies.append(pltpu.make_async_copy(o_ref.at[part], o_hbm.at[part], sem.at[g]))
        copies[-1].start()
    for copy in copies:
        copy.wait()


def stage(kernel, in_specs, out_shape, scratch, flops, nbytes, out_specs=None):
    return pl.pallas_call(
        kernel,
        in_specs=[pl.BlockSpec(memory_space=m) for m in in_specs],
        **({} if out_specs is None else {"out_specs": out_specs}),
        out_shape=out_shape,
        scratch_shapes=scratch,
        compiler_params=pltpu.CompilerParams(vmem_limit_bytes=16 * 1024 * 1024),
        cost_estimate=pl.CostEstimate(flops=flops, bytes_accessed=nbytes, transcendentals=0),
    )


def on_device(bands, spectral, coupling, quadratic):
    levels, rows, coeffs = spectral.shape
    own, cells = coupling.shape
    quarter = cells // 4
    table = trig_table(cells, coeffs)
    halves = np.stack([table[: cells // 2, : coeffs // 2], table[: cells // 2, coeffs // 2 :]])
    th, tl = (jnp.asarray(t) for t in split_table(halves))
    order = np.arange(cells).reshape(bands, own)
    order[bands // 2 :] = order[bands // 2 :, ::-1]
    ordered = np.ascontiguousarray(table[order.reshape(-1)].T)
    yh, yl = (jnp.asarray(np.stack(np.split(t, 4, 1))) for t in split_table(ordered))
    folds = np.stack([table[:quarter, f // 2 * (coeffs // 2) + f % 2 :: 2][:, : coeffs // 4] for f in range(4)])
    fh, fl = (jnp.asarray(t) for t in split_table(folds))
    bh, bl = (jnp.asarray(t) for t in split_table(np.ascontiguousarray(folds.transpose(0, 2, 1))))
    n = levels * own
    flops = 6 * n * cells * coeffs
    nbytes = 4 * n * (cells + coeffs) + 4 * cells * coeffs
    factor = (coeffs // 2) / float(cells * cells)
    spread = jax.ShapeDtypeStruct((bands, n // LANES, rows, LANES), F32)
    vmem = pltpu.VMEM

    def exchange(a):
        return lax.all_to_all(a, BAND, 0, 0, tiled=True)

    first = pl.pallas_call(
        functools.partial(synth_y, levels, rows),
        grid=(bands // 4,),
        in_specs=[
            pl.BlockSpec((levels, rows, coeffs), lambda j: (0, 0, 0)),
            pl.BlockSpec((None, coeffs, 256), lambda j: (j, 0, 0)),
            pl.BlockSpec((None, coeffs, 256), lambda j: (j, 0, 0)),
        ],
        out_specs=pl.BlockSpec((4, n // LANES, rows, LANES), lambda j: (j, 0, 0, 0)),
        out_shape=spread,
        scratch_shapes=[vmem((levels * rows, coeffs), BF16)] * 2 + [vmem((levels * rows, 256), F32)],
        compiler_params=pltpu.CompilerParams(vmem_limit_bytes=60 * 1024 * 1024),
        cost_estimate=pl.CostEstimate(flops=flops, bytes_accessed=nbytes, transcendentals=0),
    )
    second = stage(
        synth_x, [vmem] * 4,
        (jax.ShapeDtypeStruct((cells, n), F32), jax.ShapeDtypeStruct((bands, 8, LANES), F32)),
        [vmem((4, coeffs // 4, n), BF16)] * 2 + [vmem((4, quarter, 256), F32), vmem((cells, LANES), F32)],
        flops, nbytes,
    )
    third = stage(
        functools.partial(analyse_x, float(cells * cells)), [vmem] * 5, spread,
        [vmem((4, quarter, n), BF16)] * 2 + [vmem((8, n), F32), vmem((cells, LANES), F32)],
        flops, nbytes,
    )
    fourth = stage(
        functools.partial(analyse_y, levels, factor), [vmem] * 3,
        jax.ShapeDtypeStruct((levels, rows, coeffs), F32),
        [vmem((2, levels * rows, cells // 2), BF16)] * 2 + [
            vmem((levels * rows, LANES), F32), vmem((levels, rows, coeffs), F32), pltpu.SemaphoreType.DMA((PIECES,))
        ],
        flops, nbytes, pl.BlockSpec(memory_space=pl.ANY),
    )
    turned = exchange(first(spectral, yh, yl))
    product, energy = second(turned, fh, fl, coupling)
    back = exchange(third(product, exchange(energy), quadratic, bh, bl))
    return fourth(back, th, tl)


def solution(mesh):
    torus = Mesh(
        mesh.devices.reshape(mesh.shape["member"], 2, 4, 2),
        ("member",) + BAND,
    )
    return jax.shard_map(
        functools.partial(on_device, mesh.shape["band"]),
        mesh=torus,
        in_specs=(P("member", BAND, None), P(MEMBER_BAND, None), P(MEMBER_BAND, None)),
        out_specs=P("member", BAND, None),
        check_vma=False,
    )
```
